32 devices in a mesh: dp: 4 (over z), ep: 8 (over y, x, core).
Axes of the slice: x: 2, y: 2, z: 4, core: 2. Of those that a mesh axis runs over, the one named last changes fastest.
Arguments:
- hidden: bfloat16 [4096, 4096], P(('dp', 'ep')), parts along dimension 0
- k_cache: bfloat16 [4096, 32, 8, 128], P(('dp', 'ep')), parts along dimension 0
- v_cache: bfloat16 [4096, 32, 8, 128], P(('dp', 'ep')), parts along dimension 0
- seq_lens: int32 [4096], P(('dp', 'ep')), parts along dimension 0
- expert_ids: int32 [4096, 2], P(('dp', 'ep')), parts along dimension 0
- attn_gain: bfloat16 [4096], replicated
- w_query: bfloat16 [4096, 4096], replicated
- w_key: bfloat16 [4096, 1024], replicated
- w_value: bfloat16 [4096, 1024], replicated
- w_out: bfloat16 [4096, 4096], replicated
- ffn_gain: bfloat16 [4096], replicated
- w_router: bfloat16 [4096, 16], replicated
- w_gate: bfloat16 [16, 4096, 960], P('ep')
- w_up: bfloat16 [16, 4096, 960], P('ep')
- w_down: bfloat16 [16, 960, 4096], P('ep')
Outputs:
- output 1: bfloat16 [4096, 4096], P(('dp', 'ep')), parts along dimension 0
- output 2: bfloat16 [4096, 32, 8, 128], P(('dp', 'ep')), parts along dimension 0
- output 3: bfloat16 [4096, 32, 8, 128], P(('dp', 'ep')), parts along dimension 0
There are 4 independent parts. The reference program is written for one: setup_inputs(seed, part) draws one part's arguments, and reference() takes and returns one part's arrays. A program takes and returns all parts, laid end to end along the dimension named above; an argument that names none is the same for every part.
All inputs are finite; a program needn't handle non-finite values.
Results may differ from the reference program's by a relative error of at most 0.0149365.
Values are sent between devices in bfloat16 or wider.
A program may use at most 1 GiB of HBM per device.

```python
import jax
import jax.numpy as jnp
import numpy as np
from jax import lax

EP_SIZE = 8
TOK_DEV = 128
SEQ_LEN = 32
D_MODEL = 4096
D_FF = 960
Q_HEADS = 32
KV_HEADS = 8
HEAD_DIM = 128
EXPERTS = 16
TOKENS = EP_SIZE * TOK_DEV
CAP_SLOTS = 4 * TOK_DEV // EXPERTS
NORM_EPS = 1e-5
ROPE_THETA = 1000000.0


def route_pairs(rng_key):
    perm_key, tok_key, swap_key = jax.random.split(rng_key, 3)
    counts = np.array([4 * TOK_DEV // EXPERTS, TOK_DEV // EXPERTS, TOK_DEV // EXPERTS] + [2 * TOK_DEV // EXPERTS] * (EXPERTS - 3))
    rank_seq = jnp.asarray(np.repeat(np.arange(EXPERTS), counts), dtype=jnp.int32)
    expert_perm = jax.random.permutation(perm_key, EXPERTS).astype(jnp.int32)
    choice_seq = expert_perm[rank_seq]
    tok_perm = jax.random.permutation(tok_key, TOK_DEV)
    first_pick = choice_seq[:TOK_DEV][tok_perm]
    second_pick = choice_seq[TOK_DEV:][tok_perm]
    swap_bits = jax.random.randint(swap_key, (TOK_DEV,), 0, 2)
    lead_ids = jnp.where(swap_bits == 1, second_pick, first_pick)
    trail_ids = jnp.where(swap_bits == 1, first_pick, second_pick)
    return jnp.stack([lead_ids, trail_ids], axis=1)


def setup_inputs(seed: int = 0, part: int = 0) -> dict:
    root_key = jax.random.key(seed)
    part_keys = jax.random.split(jax.random.fold_in(root_key, part), 5)
    shared_keys = jax.random.split(jax.random.key(seed + 1), 10)
    q_dim = Q_HEADS * HEAD_DIM
    kv_dim = KV_HEADS * HEAD_DIM
    cache_shape = (TOKENS, SEQ_LEN, KV_HEADS, HEAD_DIM)
    hidden = jax.random.normal(part_keys[0], (TOKENS, D_MODEL), jnp.float32).astype(jnp.bfloat16)
    k_cache = (2.5 * jax.random.normal(part_keys[1], cache_shape, jnp.float32)).astype(jnp.bfloat16)
    v_cache = jax.random.normal(part_keys[2], cache_shape, jnp.float32).astype(jnp.bfloat16)
    seq_lens = jax.random.randint(part_keys[3], (TOKENS,), 0, SEQ_LEN).astype(jnp.int32).at[0].set(SEQ_LEN - 1)
    expert_ids = jax.vmap(route_pairs)(jax.random.split(part_keys[4], EP_SIZE)).reshape(TOKENS, 2)
    attn_gain = jax.random.uniform(shared_keys[0], (D_MODEL,), jnp.float32, 0.5, 1.5).astype(jnp.bfloat16)
    w_query = (jax.random.normal(shared_keys[1], (D_MODEL, q_dim), jnp.float32) * D_MODEL ** -0.5).astype(jnp.bfloat16)
    w_key = (jax.random.normal(shared_keys[2], (D_MODEL, kv_dim), jnp.float32) * D_MODEL ** -0.5).astype(jnp.bfloat16)
    w_value = (jax.random.normal(shared_keys[3], (D_MODEL, kv_dim), jnp.float32) * D_MODEL ** -0.5).astype(jnp.bfloat16)
    w_out = (jax.random.normal(shared_keys[4], (q_dim, D_MODEL), jnp.float32) * 2.0 * q_dim ** -0.5).astype(jnp.bfloat16)
    ffn_gain = jax.random.uniform(shared_keys[5], (D_MODEL,), jnp.float32, 0.5, 1.5).astype(jnp.bfloat16)
    w_router = (jax.random.normal(shared_keys[6], (D_MODEL, EXPERTS), jnp.float32) * D_MODEL ** -0.5).astype(jnp.bfloat16)
    w_gate = (jax.random.normal(shared_keys[7], (EXPERTS, D_MODEL, D_FF), jnp.float32) * D_MODEL ** -0.5).astype(jnp.bfloat16)
    w_up = (jax.random.normal(shared_keys[8], (EXPERTS, D_MODEL, D_FF), jnp.float32) * D_MODEL ** -0.5).astype(jnp.bfloat16)
    w_down = (jax.random.normal(shared_keys[9], (EXPERTS, D_FF, D_MODEL), jnp.float32) * 1.5 * D_FF ** -0.5).astype(jnp.bfloat16)
    return {'hidden': hidden, 'k_cache': k_cache, 'v_cache': v_cache, 'seq_lens': seq_lens, 'expert_ids': expert_ids, 'attn_gain': attn_gain, 'w_query': w_query, 'w_key': w_key, 'w_value': w_value, 'w_out': w_out, 'ffn_gain': ffn_gain, 'w_router': w_router, 'w_gate': w_gate, 'w_up': w_up, 'w_down': w_down}


def rms_scale(row_block, gain_vec):
    rows_f32 = row_block.astype(jnp.float32)
    inv_rms = lax.rsqrt(jnp.mean(rows_f32 * rows_f32, axis=-1, keepdims=True) + NORM_EPS)
    return (rows_f32 * inv_rms * gain_vec.astype(jnp.float32)).astype(jnp.bfloat16)


def rope_rotate(vectors, positions):
    half_dim = HEAD_DIM // 2
    inv_freq = ROPE_THETA ** (-2.0 * jnp.arange(half_dim, dtype=jnp.float32) / HEAD_DIM)
    angles = positions.astype(jnp.float32)[:, None, None] * inv_freq
    cosines = jnp.cos(angles)
    sine_vals = jnp.sin(angles)
    vec_f32 = vectors.astype(jnp.float32)
    low_half = vec_f32[..., :half_dim]
    high_half = vec_f32[..., half_dim:]
    return jnp.concatenate([low_half * cosines - high_half * sine_vals, high_half * cosines + low_half * sine_vals], axis=-1).astype(jnp.bfloat16)


def reference(hidden, k_cache, v_cache, seq_lens, expert_ids, attn_gain, w_query, w_key, w_value, w_out, ffn_gain, w_router, w_gate, w_up, w_down):
    groups = Q_HEADS // KV_HEADS
    normed = rms_scale(hidden, attn_gain)
    q_proj = jnp.dot(normed, w_query, preferred_element_type=jnp.float32).astype(jnp.bfloat16)
    q_proj = rope_rotate(q_proj.reshape(TOKENS, Q_HEADS, HEAD_DIM), seq_lens)
    key_new = jnp.dot(normed, w_key, preferred_element_type=jnp.float32).astype(jnp.bfloat16)
    key_new = rope_rotate(key_new.reshape(TOKENS, KV_HEADS, HEAD_DIM), seq_lens)
    value_new = jnp.dot(normed, w_value, preferred_element_type=jnp.float32).astype(jnp.bfloat16).reshape(TOKENS, KV_HEADS, HEAD_DIM)
    positions = jnp.arange(SEQ_LEN)
    slot_hit = (positions[None, :] == seq_lens[:, None])[:, :, None, None]
    k_cache_new = jnp.where(slot_hit, key_new[:, None], k_cache)
    v_cache_new = jnp.where(slot_hit, value_new[:, None], v_cache)

    def attend_one(operands):
        q_row, k_rows, v_rows, cur_len = operands
        q_grouped = q_row.reshape(KV_HEADS, groups, HEAD_DIM).astype(jnp.float32)
        scores = jnp.einsum('kgh,skh->kgs', q_grouped, k_rows.astype(jnp.float32)) * HEAD_DIM ** -0.5
        scores = jnp.where(positions[None, None, :] <= cur_len, scores, -jnp.inf)
        attn_probs = jax.nn.softmax(scores, axis=-1).astype(jnp.bfloat16)
        attn_mix = jnp.einsum('kgs,skh->kgh', attn_probs.astype(jnp.float32), v_rows.astype(jnp.float32))
        return attn_mix.astype(jnp.bfloat16).reshape(Q_HEADS * HEAD_DIM)

    attn_flat = lax.map(attend_one, (q_proj, k_cache_new, v_cache_new, seq_lens))
    resid_out = (hidden.astype(jnp.float32) + jnp.dot(attn_flat, w_out, preferred_element_type=jnp.float32)).astype(jnp.bfloat16)
    normed_ffn = rms_scale(resid_out, ffn_gain)
    logits = jnp.dot(normed_ffn, w_router, preferred_element_type=jnp.float32)
    gates = jax.nn.softmax(jnp.take_along_axis(logits, expert_ids, axis=1), axis=-1)
    flat_ids = expert_ids.reshape(-1)
    hit_table = (flat_ids[:, None] == jnp.arange(EXPERTS)[None, :]).astype(jnp.int32)
    slot_rank = jnp.sum((jnp.cumsum(hit_table, axis=0) - hit_table) * hit_table, axis=1)
    expert_cap = EP_SIZE * CAP_SLOTS
    flat_slot = flat_ids * expert_cap + slot_rank
    owner_tok = jnp.zeros((EXPERTS * expert_cap,), jnp.int32).at[flat_slot].set(jnp.arange(2 * TOKENS, dtype=jnp.int32) // 2)
    expert_rows = normed_ffn[owner_tok].reshape(EXPERTS, expert_cap, D_MODEL)

    def expert_ffn(operands):
        row_block, gate_mat, up_mat, down_mat = operands
        act_vals = jax.nn.silu(jnp.dot(row_block, gate_mat, preferred_element_type=jnp.float32)) * jnp.dot(row_block, up_mat, preferred_element_type=jnp.float32)
        return jnp.dot(act_vals.astype(jnp.bfloat16), down_mat, preferred_element_type=jnp.float32).astype(jnp.bfloat16)

    expert_out = lax.map(expert_ffn, (expert_rows, w_gate, w_up, w_down)).reshape(EXPERTS * expert_cap, D_MODEL)
    routed = expert_out[flat_slot].reshape(TOKENS, 2, D_MODEL).astype(jnp.float32)
    out_f32 = resid_out.astype(jnp.float32) + jnp.sum(gates[:, :, None] * routed, axis=1)
    return out_f32.astype(jnp.bfloat16), k_cache_new, v_cache_new
```

```python
import functools

import jax
import jax.numpy as jnp
from jax import lax
from jax.experimental import pallas as pl
from jax.experimental.pallas import tpu as pltpu
from jax.sharding import PartitionSpec as P

NORM_EPS = 1e-5
ROPE_THETA = 1000000.0
F32 = jnp.float32
BF16 = jnp.bfloat16
TILE = 256
RING = 4


def rope_tables(positions, head_dim):
    half_dim = head_dim // 2
    inv_freq = ROPE_THETA ** (-2.0 * jnp.arange(half_dim, dtype=F32) / head_dim)
    angles = positions.astype(F32)[:, None] * inv_freq
    cosines, sines = jnp.cos(angles), jnp.sin(angles)
    return jnp.concatenate([cosines, cosines], axis=-1), jnp.concatenate([-sines, sines], axis=-1)


def rms_rows(rows_f32, gain_row):
    inv_rms = lax.rsqrt(jnp.mean(rows_f32 * rows_f32, axis=-1, keepdims=True) + NORM_EPS)
    return (rows_f32 * inv_rms * gain_row).astype(BF16)


def qkv_kernel(x_ref, gain_ref, cos_ref, sin_ref, wq, wk, wv, out_ref, h_ref, wbuf, sems):
    head_dim = cos_ref.shape[-1]
    spans = [w.shape[1] // TILE for w in (wq, wk, wv)]
    first = [0, spans[0], spans[0] + spans[1]]
    total = sum(spans)
    per_tile = TILE // head_dim

    def start(t):
        slot = lax.rem(t, RING)
        for w, lo, n in zip((wq, wk, wv), first, spans):
            @pl.when((t >= lo) & (t < lo + n))
            def _():
                col = pl.multiple_of((t - lo) * TILE, TILE)
                pltpu.make_async_copy(w.at[:, pl.ds(col, TILE)], wbuf.at[slot], sems.at[slot]).start()

    for t in range(RING - 1):
        start(jnp.int32(t))
    h_ref[...] = rms_rows(x_ref[...].astype(F32), gain_ref[...].astype(F32))

    def step(t, carry):
        slot = lax.rem(t, RING)
        start(t + RING - 1)
        pltpu.make_async_copy(wq.at[:, pl.ds(0, TILE)], wbuf.at[slot], sems.at[slot]).wait()
        acc = jnp.dot(h_ref[...], wbuf[slot], preferred_element_type=F32)
        for i in range(per_tile):
            v = acc[:, i * head_dim:(i + 1) * head_dim].astype(BF16).astype(F32)
            rot = v * cos_ref[...] + pltpu.roll(v, head_dim // 2, 1) * sin_ref[...]
            out_ref[t * per_tile + i] = jnp.where(t < first[2], rot.astype(BF16).astype(F32), v)
        return carry

    lax.fori_loop(0, total, step, 0)


def qkv_project(hidden, gain, positions, wq, wk, wv, head_dim):
    tokens, d_model = hidden.shape
    cos, sin = rope_tables(positions, head_dim)
    heads = (wq.shape[1] + wk.shape[1] + wv.shape[1]) // head_dim
    vmem = pl.BlockSpec(memory_space=pltpu.VMEM)
    hbm = pl.BlockSpec(memory_space=pl.ANY)
    return pl.pallas_call(
        qkv_kernel,
        out_shape=jax.ShapeDtypeStruct((heads, tokens, head_dim), F32),
        in_specs=[vmem] * 4 + [hbm] * 3,
        out_specs=vmem,
        scratch_shapes=[pltpu.VMEM((tokens, d_model), BF16), pltpu.VMEM((RING, d_model, TILE), BF16), pltpu.SemaphoreType.DMA((RING,))],
        compiler_params=pltpu.CompilerParams(vmem_limit_bytes=60 << 20),
    )(hidden, gain.reshape(1, -1), cos, sin, wq, wk, wv)


def attend_kernel(lens_ref, q_ref, kn_ref, vn_ref, k_ref, v_ref, ko_ref, vo_ref, o_ref):
    block, seq_len, kv_heads, head_dim = k_ref.shape
    q_heads = q_ref.shape[0]
    groups = q_heads // kv_heads
    base = pl.program_id(0) * block
    cols = seq_len * kv_heads
    lane = lax.broadcasted_iota(jnp.int32, (q_heads, cols), 1)
    row = lax.broadcasted_iota(jnp.int32, (q_heads, cols), 0)
    pos = jnp.where(lax.rem(lane, kv_heads) == row // groups, lane // kv_heads, seq_len)
    q2 = q_ref.reshape(q_heads * block, head_dim)
    kn2 = kn_ref.reshape(kv_heads * block, head_dim)
    vn2 = vn_ref.reshape(kv_heads * block, head_dim)
    o2 = o_ref.reshape(q_heads * block, head_dim)
    ko_ref[...] = k_ref[...]
    vo_ref[...] = v_ref[...]
    lens = [lens_ref[base + t] for t in range(block)]
    for t in range(block):
        ko_ref[t, lens[t]] = kn2[pl.ds(t, kv_heads, stride=block), :].astype(BF16)
        vo_ref[t, lens[t]] = vn2[pl.ds(t, kv_heads, stride=block), :].astype(BF16)
    scores = []
    for t in range(block):
        q_t = q2[pl.ds(t, q_heads, stride=block), :].astype(BF16)
        k_t = ko_ref[t].reshape(cols, head_dim)
        scores.append(lax.dot_general(q_t, k_t, (((1,), (1,)), ((), ())), preferred_element_type=F32))
    probs = []
    for t in range(block):
        s = jnp.where(pos <= lens[t], scores[t] * head_dim ** -0.5, -jnp.inf)
        e = jnp.exp(s - jnp.max(s, axis=-1, keepdims=True))
        probs.append((e / jnp.sum(e, axis=-1, keepdims=True)).astype(BF16))
    for t in range(block):
        mix = jnp.dot(probs[t], vo_ref[t].reshape(cols, head_dim), preferred_element_type=F32)
        o2[pl.ds(t, q_heads, stride=block), :] = mix.astype(BF16).astype(F32)


def attend(qkv, k_cache, v_cache, seq_lens):
    tokens, seq_len, kv_heads, head_dim = k_cache.shape
    q_heads = qkv.shape[0] - 2 * kv_heads
    block = 8
    ratio = q_heads // kv_heads
    cache = pl.BlockSpec((block, seq_len, kv_heads, head_dim), lambda i, n: (i, 0, 0, 0))
    return pl.pallas_call(
        attend_kernel,
        grid_spec=pltpu.PrefetchScalarGridSpec(
            num_scalar_prefetch=1,
            grid=(tokens // block,),
            in_specs=[
                pl.BlockSpec((q_heads, block, head_dim), lambda i, n: (0, i, 0)),
                pl.BlockSpec((kv_heads, block, head_dim), lambda i, n: (ratio, i, 0)),
                pl.BlockSpec((kv_heads, block, head_dim), lambda i, n: (ratio + 1, i, 0)),
                cache, cache],
            out_specs=[cache, cache, pl.BlockSpec((q_heads, block, head_dim), lambda i, n: (0, i, 0))],
        ),
        out_shape=[jax.ShapeDtypeStruct(k_cache.shape, BF16), jax.ShapeDtypeStruct(v_cache.shape, BF16),
                   jax.ShapeDtypeStruct((q_heads, tokens, head_dim), F32)],
        compiler_params=pltpu.CompilerParams(vmem_limit_bytes=60 << 20),
    )(seq_lens, qkv, qkv, qkv, k_cache, v_cache)


def out_kernel(x_ref, o_ref, gain_ref, ids_ref, wr_ref, wo, x1_ref, h2_ref, gates_ref, a_ref, sq_ref, wbuf, sems):
    q_heads, tokens, head_dim = o_ref.shape
    d_model = wo.shape[1]
    total = d_model // TILE

    def copy(t):
        col = pl.multiple_of(t * TILE, TILE)
        slot = lax.rem(t, RING)
        return pltpu.make_async_copy(wo.at[:, pl.ds(col, TILE)], wbuf.at[slot], sems.at[slot])

    for t in range(RING - 1):
        copy(jnp.int32(t)).start()
    for j in range(q_heads):
        a_ref[:, j * head_dim:(j + 1) * head_dim] = o_ref[j].astype(BF16)
    sq_ref[...] = jnp.zeros_like(sq_ref)

    def step(t, carry):
        @pl.when(t + RING - 1 < total)
        def _():
            copy(t + RING - 1).start()

        copy(t).wait()
        cols = pl.ds(pl.multiple_of(t * TILE, TILE), TILE)
        acc = jnp.dot(a_ref[...], wbuf[lax.rem(t, RING)], preferred_element_type=F32)
        x1 = (x_ref[:, cols].astype(F32) + acc).astype(BF16)
        x1_ref[:, cols] = x1
        x1 = x1.astype(F32)
        sq_ref[...] += x1 * x1
        return carry

    lax.fori_loop(0, total, step, 0)
    inv = lax.rsqrt(jnp.sum(sq_ref[...], axis=-1, keepdims=True) / d_model + NORM_EPS)
    h2_ref[...] = (x1_ref[...].astype(F32) * inv * gain_ref[...].astype(F32)).astype(BF16)
    logits = jnp.dot(h2_ref[...], wr_ref[...], preferred_element_type=F32)
    expert = lax.broadcasted_iota(jnp.int32, logits.shape, 1)
    p0, p1 = (jnp.sum(jnp.where(expert == ids_ref[:, k:k + 1], logits, 0.0), axis=-1, keepdims=True) for k in range(2))
    top = jnp.maximum(p0, p1)
    e0, e1 = jnp.exp(p0 - top), jnp.exp(p1 - top)
    lane = lax.broadcasted_iota(jnp.int32, gates_ref.shape, 1)
    gates_ref[...] = jnp.where(lane == 0, e0, e1) / (e0 + e1)


def out_project(hidden, mix, ffn_gain, expert_ids, w_router, w_out):
    tokens, d_model = hidden.shape
    vmem = pl.BlockSpec(memory_space=pltpu.VMEM)
    row = jax.ShapeDtypeStruct((tokens, d_model), BF16)
    return pl.pallas_call(
        out_kernel,
        out_shape=[row, row, jax.ShapeDtypeStruct((tokens, 2), F32)],
        in_specs=[vmem] * 5 + [pl.BlockSpec(memory_space=pl.ANY)],
        out_specs=[vmem] * 3,
        scratch_shapes=[pltpu.VMEM((tokens, w_out.shape[0]), BF16), pltpu.VMEM((tokens, TILE), F32),
                        pltpu.VMEM((RING, w_out.shape[0], TILE), BF16), pltpu.SemaphoreType.DMA((RING,))],
        compiler_params=pltpu.CompilerParams(vmem_limit_bytes=60 << 20),
    )(hidden, mix, ffn_gain.reshape(1, -1), expert_ids, w_router, w_out)


def choice_slots(expert_ids, expert_list, cap_slots):
    hit_mask = expert_ids[..., None] == expert_list
    hit_counts = hit_mask.reshape(hit_mask.shape[:-3] + (-1, hit_mask.shape[-1])).astype(jnp.int32)
    before = (jnp.cumsum(hit_counts, axis=-2) - hit_counts).reshape(hit_mask.shape)
    return (hit_mask[..., None] & (before[..., None] == jnp.arange(cap_slots))).astype(jnp.bfloat16)


def solution(mesh):
    n_ep = mesh.shape['ep']
    row_spec = P(('dp', 'ep'), None)
    cache_spec = P(('dp', 'ep'), None, None, None)
    expert_spec = P('ep', None, None)
    in_specs = (row_spec, cache_spec, cache_spec, P(('dp', 'ep')), row_spec, P(), P(), P(), P(), P(), P(), P(), expert_spec, expert_spec, expert_spec)
    out_specs = (row_spec, cache_spec, cache_spec)

    def device_step(hidden, k_cache, v_cache, seq_lens, expert_ids, attn_gain, w_query, w_key, w_value, w_out, ffn_gain, w_router, w_gate, w_up, w_down):
        tokens, d_model = hidden.shape
        local_experts = w_gate.shape[0]
        n_experts = local_experts * n_ep
        cap_slots = 4 * tokens // n_experts
        head_dim = k_cache.shape[-1]
        qkv = qkv_project(hidden, attn_gain, seq_lens, w_query, w_key, w_value, head_dim)
        k_cache_new, v_cache_new, mix = attend(qkv, k_cache, v_cache, seq_lens)
        resid_out, normed_ffn, gates = out_project(hidden, mix, ffn_gain, expert_ids, w_router, w_out)
        slot_sel = choice_slots(expert_ids, jnp.arange(n_experts), cap_slots)
        send_buf = jnp.einsum('tkec,td->ecd', slot_sel, normed_ffn, preferred_element_type=jnp.float32).astype(jnp.bfloat16)
        send_buf = send_buf.reshape(n_ep, local_experts, cap_slots, d_model)
        recv_buf = lax.all_to_all(send_buf, 'ep', 0, 0, tiled=True)
        gate_act = jnp.einsum('sxcd,xdf->sxcf', recv_buf, w_gate, preferred_element_type=jnp.float32)
        up_act = jnp.einsum('sxcd,xdf->sxcf', recv_buf, w_up, preferred_element_type=jnp.float32)
        inner_act = (jax.nn.silu(gate_act) * up_act).astype(jnp.bfloat16)
        expert_out = jnp.einsum('sxcf,xfd->sxcd', inner_act, w_down, preferred_element_type=jnp.float32).astype(jnp.bfloat16)
        returned = lax.all_to_all(expert_out, 'ep', 0, 0, tiled=True).reshape(n_experts, cap_slots, d_model)
        routed = jnp.einsum('tkec,ecd->tkd', slot_sel, returned, preferred_element_type=jnp.float32)
        out_f32 = resid_out.astype(jnp.float32) + jnp.sum(gates[:, :, None] * routed, axis=1)
        return out_f32.astype(jnp.bfloat16), k_cache_new, v_cache_new

    return jax.shard_map(device_step, mesh=mesh, in_specs=in_specs, out_specs=out_specs, check_vma=False)
```

```python
import functools

import jax
import jax.numpy as jnp
from jax import lax
from jax.experimental import pallas as pl
from jax.experimental.pallas import tpu as pltpu
from jax.sharding import PartitionSpec as P

NORM_EPS = 1e-5
ROPE_THETA = 1000000.0
F32 = jnp.float32
BF16 = jnp.bfloat16
TILE = 256
RING = 4
CHUNKS = 4


def rope_tables(positions, head_dim):
    half_dim = head_dim // 2
    inv_freq = ROPE_THETA ** (-2.0 * jnp.arange(half_dim, dtype=F32) / head_dim)
    angles = positions.astype(F32)[:, None] * inv_freq
    cosines, sines = jnp.cos(angles), jnp.sin(angles)
    return jnp.concatenate([cosines, cosines], axis=-1), jnp.concatenate([-sines, sines], axis=-1)


def rms_rows(rows_f32, gain_row):
    inv_rms = lax.rsqrt(jnp.mean(rows_f32 * rows_f32, axis=-1, keepdims=True) + NORM_EPS)
    return (rows_f32 * inv_rms * gain_row).astype(BF16)


def qkv_kernel(x_ref, gain_ref, cos_ref, sin_ref, wq, wk, wv, out_ref, h_ref, wbuf, sems):
    head_dim = cos_ref.shape[-1]
    spans = [w.shape[1] // TILE for w in (wq, wk, wv)]
    first = [0, spans[0], spans[0] + spans[1]]
    total = sum(spans)
    per_tile = TILE // head_dim

    def start(t):
        slot = lax.rem(t, RING)
        for w, lo, n in zip((wq, wk, wv), first, spans):
            @pl.when((t >= lo) & (t < lo + n))
            def _():
                col = pl.multiple_of((t - lo) * TILE, TILE)
                pltpu.make_async_copy(w.at[:, pl.ds(col, TILE)], wbuf.at[slot], sems.at[slot]).start()

    for t in range(RING - 1):
        start(jnp.int32(t))
    h_ref[...] = rms_rows(x_ref[...].astype(F32), gain_ref[...].astype(F32))

    def step(t, carry):
        slot = lax.rem(t, RING)
        start(t + RING - 1)
        pltpu.make_async_copy(wq.at[:, pl.ds(0, TILE)], wbuf.at[slot], sems.at[slot]).wait()
        acc = jnp.dot(h_ref[...], wbuf[slot], preferred_element_type=F32)
        for i in range(per_tile):
            v = acc[:, i * head_dim:(i + 1) * head_dim].astype(BF16).astype(F32)
            rot = v * cos_ref[...] + pltpu.roll(v, head_dim // 2, 1) * sin_ref[...]
            out_ref[t * per_tile + i] = jnp.where(t < first[2], rot.astype(BF16).astype(F32), v)
        return carry

    lax.fori_loop(0, total, step, 0)


def qkv_project(hidden, gain, positions, wq, wk, wv, head_dim):
    tokens, d_model = hidden.shape
    cos, sin = rope_tables(positions, head_dim)
    heads = (wq.shape[1] + wk.shape[1] + wv.shape[1]) // head_dim
    vmem = pl.BlockSpec(memory_space=pltpu.VMEM)
    hbm = pl.BlockSpec(memory_space=pl.ANY)
    return pl.pallas_call(
        qkv_kernel,
        out_shape=jax.ShapeDtypeStruct((heads, tokens, head_dim), F32),
        in_specs=[vmem] * 4 + [hbm] * 3,
        out_specs=vmem,
        scratch_shapes=[pltpu.VMEM((tokens, d_model), BF16), pltpu.VMEM((RING, d_model, TILE), BF16), pltpu.SemaphoreType.DMA((RING,))],
        compiler_params=pltpu.CompilerParams(vmem_limit_bytes=60 << 20),
    )(hidden, gain.reshape(1, -1), cos, sin, wq, wk, wv)


def attend_kernel(lens_ref, q_ref, kn_ref, vn_ref, k_ref, v_ref, ko_ref, vo_ref, o_ref):
    block, seq_len, kv_heads, head_dim = k_ref.shape
    q_heads = q_ref.shape[0]
    groups = q_heads // kv_heads
    base = pl.program_id(0) * block
    cols = seq_len * kv_heads
    lane = lax.broadcasted_iota(jnp.int32, (q_heads, cols), 1)
    row = lax.broadcasted_iota(jnp.int32, (q_heads, cols), 0)
    pos = jnp.where(lax.rem(lane, kv_heads) == row // groups, lane // kv_heads, seq_len)
    q2 = q_ref.reshape(q_heads * block, head_dim)
    kn2 = kn_ref.reshape(kv_heads * block, head_dim)
    vn2 = vn_ref.reshape(kv_heads * block, head_dim)
    o2 = o_ref.reshape(q_heads * block, head_dim)
    ko_ref[...] = k_ref[...]
    vo_ref[...] = v_ref[...]
    lens = [lens_ref[base + t] for t in range(block)]
    for t in range(block):
        ko_ref[t, lens[t]] = kn2[pl.ds(t, kv_heads, stride=block), :].astype(BF16)
        vo_ref[t, lens[t]] = vn2[pl.ds(t, kv_heads, stride=block), :].astype(BF16)
    scores = []
    for t in range(block):
        q_t = q2[pl.ds(t, q_heads, stride=block), :].astype(BF16)
        k_t = ko_ref[t].reshape(cols, head_dim)
        scores.append(lax.dot_general(q_t, k_t, (((1,), (1,)), ((), ())), preferred_element_type=F32))
    probs = []
    for t in range(block):
        s = jnp.where(pos <= lens[t], scores[t] * head_dim ** -0.5, -jnp.inf)
        e = jnp.exp(s - jnp.max(s, axis=-1, keepdims=True))
        probs.append((e / jnp.sum(e, axis=-1, keepdims=True)).astype(BF16))
    for t in range(block):
        mix = jnp.dot(probs[t], vo_ref[t].reshape(cols, head_dim), preferred_element_type=F32)
        o2[pl.ds(t, q_heads, stride=block), :] = mix.astype(BF16).astype(F32)


def attend(qkv, k_cache, v_cache, seq_lens):
    tokens, seq_len, kv_heads, head_dim = k_cache.shape
    q_heads = qkv.shape[0] - 2 * kv_heads
    block = 8
    ratio = q_heads // kv_heads
    cache = pl.BlockSpec((block, seq_len, kv_heads, head_dim), lambda i, n: (i, 0, 0, 0))
    return pl.pallas_call(
        attend_kernel,
        grid_spec=pltpu.PrefetchScalarGridSpec(
            num_scalar_prefetch=1,
            grid=(tokens // block,),
            in_specs=[
                pl.BlockSpec((q_heads, block, head_dim), lambda i, n: (0, i, 0)),
                pl.BlockSpec((kv_heads, block, head_dim), lambda i, n: (ratio, i, 0)),
                pl.BlockSpec((kv_heads, block, head_dim), lambda i, n: (ratio + 1, i, 0)),
                cache, cache],
            out_specs=[cache, cache, pl.BlockSpec((q_heads, block, head_dim), lambda i, n: (0, i, 0))],
        ),
        out_shape=[jax.ShapeDtypeStruct(k_cache.shape, BF16), jax.ShapeDtypeStruct(v_cache.shape, BF16),
                   jax.ShapeDtypeStruct((q_heads, tokens, head_dim), F32)],
        compiler_params=pltpu.CompilerParams(vmem_limit_bytes=60 << 20),
    )(seq_lens, qkv, qkv, qkv, k_cache, v_cache)


def out_kernel(x_ref, o_ref, gain_ref, ids_ref, wr_ref, wo, x1_ref, h2_ref, gates_ref, a_ref, sq_ref, wbuf, sems):
    q_heads, tokens, head_dim = o_ref.shape
    d_model = wo.shape[1]
    total = d_model // TILE

    def copy(t):
        col = pl.multiple_of(t * TILE, TILE)
        slot = lax.rem(t, RING)
        return pltpu.make_async_copy(wo.at[:, pl.ds(col, TILE)], wbuf.at[slot], sems.at[slot])

    for t in range(RING - 1):
        copy(jnp.int32(t)).start()
    for j in range(q_heads):
        a_ref[:, j * head_dim:(j + 1) * head_dim] = o_ref[j].astype(BF16)
    sq_ref[...] = jnp.zeros_like(sq_ref)

    def step(t, carry):
        @pl.when(t + RING - 1 < total)
        def _():
            copy(t + RING - 1).start()

        copy(t).wait()
        cols = pl.ds(pl.multiple_of(t * TILE, TILE), TILE)
        acc = jnp.dot(a_ref[...], wbuf[lax.rem(t, RING)], preferred_element_type=F32)
        x1 = (x_ref[:, cols].astype(F32) + acc).astype(BF16)
        x1_ref[:, cols] = x1
        x1 = x1.astype(F32)
        sq_ref[...] += x1 * x1
        return carry

    lax.fori_loop(0, total, step, 0)
    inv = lax.rsqrt(jnp.sum(sq_ref[...], axis=-1, keepdims=True) / d_model + NORM_EPS)
    chunks, _, width = h2_ref.shape
    logits = jnp.zeros((tokens, wr_ref.shape[0]), F32)
    for q in range(chunks):
        cols = slice(q * width, (q + 1) * width)
        h2_ref[q] = (x1_ref[:, cols].astype(F32) * inv * gain_ref[:, cols].astype(F32)).astype(BF16)
        logits += lax.dot_general(h2_ref[q], wr_ref[:, cols], (((1,), (1,)), ((), ())), preferred_element_type=F32)
    expert = lax.broadcasted_iota(jnp.int32, logits.shape, 1)
    p0, p1 = (jnp.sum(jnp.where(expert == ids_ref[:, k:k + 1], logits, 0.0), axis=-1, keepdims=True) for k in range(2))
    top = jnp.maximum(p0, p1)
    e0, e1 = jnp.exp(p0 - top), jnp.exp(p1 - top)
    lane = lax.broadcasted_iota(jnp.int32, gates_ref.shape, 1)
    gates_ref[...] = jnp.where(lane == 0, e0, e1) / (e0 + e1)


def out_project(hidden, mix, ffn_gain, expert_ids, w_router, w_out):
    tokens, d_model = hidden.shape
    vmem = pl.BlockSpec(memory_space=pltpu.VMEM)
    row = jax.ShapeDtypeStruct((tokens, d_model), BF16)
    return pl.pallas_call(
        out_kernel,
        out_shape=[row, jax.ShapeDtypeStruct((CHUNKS, tokens, d_model // CHUNKS), BF16), jax.ShapeDtypeStruct((tokens, 2), F32)],
        in_specs=[vmem] * 5 + [pl.BlockSpec(memory_space=pl.ANY)],
        out_specs=[vmem] * 3,
        scratch_shapes=[pltpu.VMEM((tokens, w_out.shape[0]), BF16), pltpu.VMEM((tokens, TILE), F32),
                        pltpu.VMEM((RING, w_out.shape[0], TILE), BF16), pltpu.SemaphoreType.DMA((RING,))],
        compiler_params=pltpu.CompilerParams(vmem_limit_bytes=60 << 20),
    )(hidden, mix, ffn_gain.reshape(1, -1), expert_ids, w_router.T, w_out)


def moe_kernel(n_ep, h_ref, x1_ref, gates_ref, codes_ref, code_cols_ref, wg, wu, wd, out_ref,
               buf, x_ref, y_in, act_ref, sum_ref, codes_in, wbuf, wsem, csend, crecv, gsend, grecv, ysend, yrecv):
    me = lax.axis_index('ep')
    bits = [lax.rem(me, 2), lax.rem(me // 2, 2), me // 4]
    chunks, tokens, width = h_ref.shape
    d_model = chunks * width
    local_experts, rows_all, _ = x_ref.shape
    cap = rows_all // n_ep
    d_ff = wd.shape[1]

    def peer(r):
        return me + sum(((r >> b) & 1) * (1 << b) * (1 - 2 * bits[b]) for b in range(3))

    def remote(src, dst, send, recv, r):
        return pltpu.make_async_remote_copy(src_ref=src, dst_ref=dst, send_sem=send, recv_sem=recv, device_id={'ep': peer(r)},
                                            device_id_type=pl.DeviceIdType.MESH)

    def block(r, q):
        return h_ref.at[q] if r == 0 else buf.at[r - 1, q]

    def push(slot, q):
        if slot in (2, 4):
            src, to = 0, slot
        elif slot == 6:
            src, to = (2, 4) if q < chunks // 2 else (4, 2)
        else:
            src, to = slot - 1, 1
        return remote(block(src, q), buf.at[slot - 1, q], gsend.at[slot, q], grecv.at[slot, q], to)

    def weight(i):
        e, m = i // 3, i % 3
        slot = i if i < 5 else 0
        return pltpu.make_async_copy((wg, wu, wd)[m].at[e], wbuf.at[slot], wsem.at[i])

    def code_copy(r):
        return remote(codes_ref, codes_in.at[r], csend.at[r], crecv.at[r], r)

    for i in range(5):
        weight(i).start()
    barrier = pltpu.get_barrier_semaphore()
    for r in range(1, n_ep):
        pl.semaphore_signal(barrier, inc=1, device_id={'ep': peer(r)}, device_id_type=pl.DeviceIdType.MESH)
    pl.semaphore_wait(barrier, n_ep - 1)

    for r in range(1, n_ep):
        code_copy(r).start()
    for q in range(chunks):
        push(2, q).start()
        push(4, q).start()
    for q in range(chunks):
        push(1, q).start()

    slot_iota = lax.broadcasted_iota(jnp.int32, (local_experts * cap, tokens), 0)
    picks = {}

    def select(r, q):
        if r not in picks:
            if r:
                code_copy(r).wait_recv()
            codes = codes_ref[...] if r == 0 else codes_in[r]
            want = (slot_iota + me * (local_experts * cap)).astype(F32)
            hit = (jnp.broadcast_to(codes[0:1], want.shape) == want) | (jnp.broadcast_to(codes[1:2], want.shape) == want)
            picks[r] = jnp.where(hit, 1.0, 0.0).astype(BF16)
        got = jnp.dot(picks[r], block(r, q)[...], preferred_element_type=F32).astype(BF16)
        for e in range(local_experts):
            x_ref[e, r * cap:(r + 1) * cap, q * width:(q + 1) * width] = got[e * cap:(e + 1) * cap]

    for q in range(chunks):
        select(0, q)
    for q in range(chunks):
        for slot in (2, 4):
            push(slot, q).wait_recv()
            if (slot == 2) == (q < chunks // 2):
                push(6, q).start()
            push(slot + 1, q).start()
        for slot in (1, 2, 4):
            if slot == 1:
                push(slot, q).wait_recv()
            select(slot, q)
    for q in range(chunks):
        for slot in (3, 5):
            push(slot, q).wait_recv()
            select(slot, q)
    for q in (0, chunks // 2, 1, chunks // 2 + 1):
        push(6, q).wait_recv()
        push(7, q).start()
        select(6, q)
    for q in (0, chunks // 2, 1, chunks // 2 + 1):
        push(7, q).wait_recv()
        select(7, q)

    def y_copy(e, r):
        rows = pl.ds(r * cap, cap)
        return remote(x_ref.at[e, rows], y_in.at[e, rows], ysend.at[e, r], yrecv.at[e, r], r)

    order = (6, 7, 2, 4, 3, 5, 1)
    for e in range(local_experts):
        base = 3 * e
        slots = [i if i < 5 else 0 for i in range(base, base + 3)]
        weight(base).wait()
        weight(base + 1).wait()
        for lo in range(0, d_ff, 256):
            hi = min(lo + 256, d_ff)
            gate, up = (lax.dot_general(x_ref[e], wbuf[s, lo:hi], (((1,), (1,)), ((), ())), preferred_element_type=F32) for s in slots[:2])
            act_ref[:, lo:hi] = (gate * jax.nn.sigmoid(gate) * up).astype(BF16)
        if e == 0:
            weight(5).start()
        weight(base + 2).wait()
        for lo in range(0, d_model, 512):
            x_ref[e, :, lo:lo + 512] = jnp.dot(act_ref[...], wbuf[slots[2], :, lo:lo + 512], preferred_element_type=F32).astype(BF16)
        for r in order:
            y_copy(e, r).start()
        y_in[e, 0:cap] = x_ref[e, 0:cap]

    lane = lax.broadcasted_iota(jnp.int32, (tokens, rows_all), 1)
    rel, rank = lane // cap, lax.rem(lane, cap)
    owner = me + sum(lax.rem(rel // (1 << b), 2) * (1 << b) * (1 - 2 * bits[b]) for b in range(3))
    for e in range(local_experts):
        for r in range(1, n_ep):
            y_copy(e, r).wait_recv()
        want = ((owner * local_experts + e) * cap + rank).astype(F32)
        sel = [jnp.where(code_cols_ref[:, k:k + 1] == want, 1.0, 0.0).astype(BF16) for k in range(2)]
        for lo in range(0, d_model, 512):
            y = y_in[e, :, lo:lo + 512]
            part = sum(gates_ref[:, k:k + 1] * jnp.dot(sel[k], y, preferred_element_type=F32) for k in range(2))
            if e < local_experts - 1:
                sum_ref[:, lo:lo + 512] = part
            else:
                out_ref[:, lo:lo + 512] = (x1_ref[:, lo:lo + 512].astype(F32) + (sum_ref[:, lo:lo + 512] + part)).astype(BF16)

    for r in range(1, n_ep):
        code_copy(r).wait_send()
        for q in range(chunks):
            push(r, q).wait_send()
        for e in range(local_experts):
            y_copy(e, r).wait_send()


def moe(h2, x1, gates, expert_ids, w_gate, w_up, w_down, n_ep, cap):
    chunks, tokens, width = h2.shape
    d_model = chunks * width
    local_experts, d_ff, _ = w_down.shape
    hits = (expert_ids[:, :, None] == jnp.arange(n_ep * local_experts)).astype(F32)
    counts = jnp.sum(hits, axis=1)
    before = jnp.dot(jnp.tril(jnp.ones((tokens, tokens), F32), -1), counts, precision=lax.Precision.HIGHEST)
    code_cols = expert_ids.astype(F32) * cap + jnp.sum(hits * before[:, None, :], axis=-1)
    codes = jnp.zeros((8, tokens), F32).at[:2].set(code_cols.T)
    vmem = pl.BlockSpec(memory_space=pltpu.VMEM)
    hbm = pl.BlockSpec(memory_space=pl.ANY)
    rows = n_ep * cap
    dma = pltpu.SemaphoreType.DMA
    return pl.pallas_call(
        functools.partial(moe_kernel, n_ep),
        out_shape=jax.ShapeDtypeStruct((tokens, d_model), BF16),
        in_specs=[vmem] * 5 + [hbm] * 3,
        out_specs=vmem,
        scratch_shapes=[
            pltpu.VMEM((n_ep - 1, chunks, tokens, width), BF16),
            pltpu.VMEM((local_experts, rows, d_model), BF16),
            pltpu.VMEM((local_experts, rows, d_model), BF16),
            pltpu.VMEM((rows, d_ff), BF16),
            pltpu.VMEM((tokens, d_model), F32),
            pltpu.VMEM((n_ep, 8, tokens), F32),
            pltpu.VMEM((5, d_ff, d_model), BF16),
            dma((6,)), dma((n_ep,)), dma((n_ep,)), dma((n_ep, chunks)), dma((n_ep, chunks)), dma((local_experts, n_ep)), dma((local_experts, n_ep)),
        ],
        compiler_params=pltpu.CompilerParams(vmem_limit_bytes=67043328, collective_id=0, has_side_effects=True),
    )(h2, x1, gates, codes, code_cols, jnp.swapaxes(w_gate, 1, 2), jnp.swapaxes(w_up, 1, 2), w_down)


def solution(mesh):
    n_ep = mesh.shape['ep']
    row_spec = P(('dp', 'ep'), None)
    cache_spec = P(('dp', 'ep'), None, None, None)
    expert_spec = P('ep', None, None)
    in_specs = (row_spec, cache_spec, cache_spec, P(('dp', 'ep')), row_spec, P(), P(), P(), P(), P(), P(), P(), expert_spec, expert_spec, expert_spec)
    out_specs = (row_spec, cache_spec, cache_spec)

    def device_step(hidden, k_cache, v_cache, seq_lens, expert_ids, attn_gain, w_query, w_key, w_value, w_out, ffn_gain, w_router, w_gate, w_up, w_down):
        tokens, d_model = hidden.shape
        local_experts = w_gate.shape[0]
        n_experts = local_experts * n_ep
        cap_slots = 4 * tokens // n_experts
        head_dim = k_cache.shape[-1]
        qkv = qkv_project(hidden, attn_gain, seq_lens, w_query, w_key, w_value, head_dim)
        k_cache_new, v_cache_new, mix = attend(qkv, k_cache, v_cache, seq_lens)
        resid_out, normed_ffn, gates = out_project(hidden, mix, ffn_gain, expert_ids, w_router, w_out)
        out = moe(normed_ffn, resid_out, gates, expert_ids, w_gate, w_up, w_down, n_ep, cap_slots)
        return out, k_cache_new, v_cache_new

    return jax.shard_map(device_step, mesh=mesh, in_specs=in_specs, out_specs=out_specs, check_vma=False)
```

```python
import functools

import jax
import jax.numpy as jnp
from jax import lax
from jax.experimental import pallas as pl
from jax.experimental.pallas import tpu as pltpu
from jax.sharding import PartitionSpec as P

NORM_EPS = 1e-5
ROPE_THETA = 1000000.0
F32 = jnp.float32
BF16 = jnp.bfloat16
TILE = 256
RING = 12
CHUNKS = 4


def rms_rows(rows_f32, gain_row):
    inv_rms = lax.rsqrt(jnp.mean(rows_f32 * rows_f32, axis=-1, keepdims=True) + NORM_EPS)
    return (rows_f32 * inv_rms * gain_row).astype(BF16)


def attend_kernel(lens_ref, x_ref, gain_ref, freq_ref, wq, wk, wv, k_hbm, v_hbm, ko_hbm, vo_hbm, mix_ref,
                  h_ref, cos_ref, sin_ref, qkv_ref, o_ref, kc, vc, wbuf, wsems, in_sems, out_sems):
    tokens, seq_len, kv_heads, head_dim = kc.shape
    q_heads = wq.shape[1] // head_dim
    groups = q_heads // kv_heads
    spans = [w.shape[1] // TILE for w in (wq, wk, wv)]
    first = [0, spans[0], spans[0] + spans[1]]
    total = sum(spans)
    per_tile = TILE // head_dim
    n_parts = in_sems.shape[1]
    part = tokens // n_parts
    block = o_ref.shape[1]

    def cache_in(i, w):
        rows = pl.ds(i * part, part)
        return pltpu.make_async_copy((k_hbm, v_hbm)[w].at[rows], (kc, vc)[w].at[rows], in_sems.at[w, i])

    def cache_out(i, w):
        rows = pl.ds(i * part, part)
        return pltpu.make_async_copy((kc, vc)[w].at[rows], (ko_hbm, vo_hbm)[w].at[rows], out_sems.at[w, i])

    def start(t):
        slot = lax.rem(t, RING)
        for w, lo, n in zip((wq, wk, wv), first, spans):
            @pl.when((t >= lo) & (t < lo + n))
            def _():
                col = pl.multiple_of((t - lo) * TILE, TILE)
                pltpu.make_async_copy(w.at[:, pl.ds(col, TILE)], wbuf.at[slot], wsems.at[slot]).start()

        @pl.when((t >= total) & (t < total + n_parts))
        def _():
            for w in range(2):
                cache_in(t - total, w).start()

    for t in range(RING - 1):
        start(jnp.int32(t))
    h_ref[...] = rms_rows(x_ref[...].astype(F32), gain_ref[...].astype(F32).reshape(1, -1))

    def fill(t, carry):
        cos_ref[pl.ds(t, 1), :] = jnp.full((1, head_dim), lens_ref[t].astype(F32))
        return carry

    lax.fori_loop(0, tokens, fill, 0)
    angles = cos_ref[...] * freq_ref[...]
    lane = lax.broadcasted_iota(jnp.int32, angles.shape, 1)
    sines = jnp.sin(angles)
    cos_ref[...] = jnp.cos(angles)
    sin_ref[...] = jnp.where(lane < head_dim // 2, -sines, sines)

    def project(t, carry):
        slot = lax.rem(t, RING)
        start(t + RING - 1)
        pltpu.make_async_copy(wq.at[:, pl.ds(0, TILE)], wbuf.at[slot], wsems.at[slot]).wait()
        acc = jnp.dot(h_ref[...], wbuf[slot], preferred_element_type=F32)
        for i in range(per_tile):
            v = acc[:, i * head_dim:(i + 1) * head_dim].astype(BF16).astype(F32)
            rot = v * cos_ref[...] + pltpu.roll(v, head_dim // 2, 1) * sin_ref[...]
            qkv_ref[t * per_tile + i] = jnp.where(t < first[2], rot.astype(BF16).astype(F32), v)
        return carry

    lax.fori_loop(0, total, project, 0)

    cols = seq_len * kv_heads
    lane = lax.broadcasted_iota(jnp.int32, (q_heads, cols), 1)
    row = lax.broadcasted_iota(jnp.int32, (q_heads, cols), 0)
    pos = jnp.where(lax.rem(lane, kv_heads) == row // groups, lane // kv_heads, seq_len)
    flat = qkv_ref.reshape(qkv_ref.shape[0] * tokens, head_dim)
    o2 = o_ref.reshape(q_heads * block, head_dim)

    def heads_of(t, lo, n):
        return flat[pl.ds(lo * tokens + t, n, stride=tokens), :].astype(BF16)

    def attend_part(i, carry):
        for w in range(2):
            cache_in(i, w).wait()
        for b in range(part // block):
            base = i * part + b * block
            lens = [lens_ref[base + t] for t in range(block)]
            for t in range(block):
                kc[base + t, lens[t]] = heads_of(base + t, q_heads, kv_heads)
                vc[base + t, lens[t]] = heads_of(base + t, q_heads + kv_heads, kv_heads)
            scores = [lax.dot_general(heads_of(base + t, 0, q_heads), kc[base + t].reshape(cols, head_dim),
                                      (((1,), (1,)), ((), ())), preferred_element_type=F32) for t in range(block)]
            probs = []
            for t in range(block):
                s = jnp.where(pos <= lens[t], scores[t] * head_dim ** -0.5, -jnp.inf)
                e = jnp.exp(s - jnp.max(s, axis=-1, keepdims=True))
                probs.append((e / jnp.sum(e, axis=-1, keepdims=True)).astype(BF16))
            for t in range(block):
                o2[pl.ds(t, q_heads, stride=block), :] = jnp.dot(probs[t], vc[base + t].reshape(cols, head_dim), preferred_element_type=F32)
            rows = pl.ds(pl.multiple_of(base, block), block)
            for j in range(q_heads):
                mix_ref[rows, j * head_dim:(j + 1) * head_dim] = o_ref[j].astype(BF16)
        for w in range(2):
            cache_out(i, w).start()
        return carry

    for t in range(total + RING - 1, total + n_parts):
        start(jnp.int32(t))
    lax.fori_loop(0, n_parts, attend_part, 0)
    for i in range(n_parts):
        for w in range(2):
            cache_out(i, w).wait()


def attend(hidden, gain, positions, wq, wk, wv, k_cache, v_cache):
    tokens, d_model = hidden.shape
    seq_len, kv_heads, head_dim = k_cache.shape[1:]
    q_dim = wq.shape[1]
    q_heads = q_dim // head_dim
    half_dim = head_dim // 2
    inv_freq = ROPE_THETA ** (-2.0 * jnp.arange(half_dim, dtype=F32) / head_dim)
    freq = jnp.concatenate([inv_freq, inv_freq]).reshape(1, head_dim)
    parts, block = 8, 8
    vmem = pl.BlockSpec(memory_space=pltpu.VMEM)
    hbm = pl.BlockSpec(memory_space=pl.ANY)
    dma = pltpu.SemaphoreType.DMA
    return pl.pallas_call(
        attend_kernel,
        out_shape=[jax.ShapeDtypeStruct(k_cache.shape, BF16), jax.ShapeDtypeStruct(v_cache.shape, BF16),
                   jax.ShapeDtypeStruct((tokens, q_dim), BF16)],
        in_specs=[pl.BlockSpec(memory_space=pltpu.SMEM), vmem, vmem, vmem] + [hbm] * 5,
        out_specs=[hbm, hbm, vmem],
        scratch_shapes=[
            pltpu.VMEM((tokens, d_model), BF16), pltpu.VMEM((tokens, head_dim), F32), pltpu.VMEM((tokens, head_dim), F32),
            pltpu.VMEM((q_heads + 2 * kv_heads, tokens, head_dim), F32), pltpu.VMEM((q_heads, block, head_dim), F32),
            pltpu.VMEM(k_cache.shape, BF16), pltpu.VMEM(v_cache.shape, BF16),
            pltpu.VMEM((RING, d_model, TILE), BF16),
            dma((RING,)), dma((2, parts)), dma((2, parts)),
        ],
        compiler_params=pltpu.CompilerParams(vmem_limit_bytes=67043328),
    )(positions, hidden, gain, freq, wq, wk, wv, k_cache, v_cache)


def moe_kernel(n_ep, n_experts, cap, x_in, mix_ref, gain_ref, wr_ref, ids_ref, wo, wg, wu, wd, out_ref,
               h_ref, buf, x_ref, y_in, act_ref, sum_ref, gates_ref, cols_ref, meta_ref, meta_in, wbuf,
               osem, wsem, csend, crecv, gsend, grecv, ysend, yrecv):
    me = lax.axis_index('ep')
    bits = [lax.rem(me, 2), lax.rem(me // 2, 2), me // 4]
    chunks, tokens, width = h_ref.shape
    d_model = chunks * width
    local_experts, rows_all, _ = x_ref.shape
    d_ff = wd.shape[1]
    q_dim = wo.shape[0]

    def peer(r):
        return me + sum(((r >> b) & 1) * (1 << b) * (1 - 2 * bits[b]) for b in range(3))

    def remote(src, dst, send, recv, r):
        return pltpu.make_async_remote_copy(src_ref=src, dst_ref=dst, send_sem=send, recv_sem=recv, device_id={'ep': peer(r)},
                                            device_id_type=pl.DeviceIdType.MESH)

    def block(r, q):
        return h_ref.at[q] if r == 0 else buf.at[r - 1, q]

    def push(slot, q):
        if slot in (2, 4):
            src, to = 0, slot
        elif slot == 6:
            src, to = (2, 4) if q < chunks // 2 else (4, 2)
        else:
            src, to = slot - 1, 1
        return remote(block(src, q), buf.at[slot - 1, q], gsend.at[slot, q], grecv.at[slot, q], to)

    groups = 8
    piece = q_dim // groups

    def piece_at(c, g):
        return wbuf.at[2 * (c % 2) + g // 4, 0:piece, (g % 4) * width:(g % 4 + 1) * width]

    def piece_copy(c, g):
        return pltpu.make_async_copy(wo.at[g * piece:(g + 1) * piece, c * width:(c + 1) * width], piece_at(c, g), osem.at[(c % 2) * groups + g])

    loads = ((0, 0, 4), (1, 0, 0), (2, 0, 1), (0, 1, 2), (1, 1, 3), (2, 1, 4), (0, 0, 2))

    def weight(i):
        m, e, slot = loads[i]
        return pltpu.make_async_copy((wg, wu, wd)[m].at[e], wbuf.at[slot], wsem.at[i])

    def meta_copy(r):
        return remote(meta_ref, meta_in.at[r], csend.at[r], crecv.at[r], r)

    for c in range(2):
        for g in range(groups):
            piece_copy(c, g).start()
    barrier = pltpu.get_barrier_semaphore()
    for r in range(1, n_ep):
        pl.semaphore_signal(barrier, inc=1, device_id={'ep': peer(r)}, device_id_type=pl.DeviceIdType.MESH)

    expert = lax.broadcasted_iota(jnp.int32, (n_experts, tokens), 0)
    hits = [jnp.where(jnp.broadcast_to(ids_ref[k:k + 1, :], expert.shape) == expert, 1.0, 0.0) for k in range(2)]
    earlier = lax.broadcasted_iota(jnp.int32, (tokens, tokens), 0) < lax.broadcasted_iota(jnp.int32, (tokens, tokens), 1)
    before = jnp.dot((hits[0] + hits[1]).astype(BF16), jnp.where(earlier, 1.0, 0.0).astype(BF16), preferred_element_type=F32)
    code = [ids_ref[k:k + 1, :].astype(F32) * cap + jnp.sum(hits[k] * before, axis=0, keepdims=True) for k in range(2)]
    meta_ref[...] = jnp.concatenate([jnp.broadcast_to(c, (1, tokens)) for c in code] + [jnp.zeros((6, tokens), F32)], axis=0)
    cols_ref[...] = jnp.concatenate([meta_ref[...]] * (tokens // 8), axis=0).T

    pl.semaphore_wait(barrier, n_ep - 1)

    square = jnp.zeros((tokens, 1), F32)
    for c in range(chunks):
        for g in range(groups):
            piece_copy(c, g).wait()
        for lo in range(0, width, 256):
            acc = sum(jnp.dot(mix_ref[:, g * piece:(g + 1) * piece],
                              wbuf[2 * (c % 2) + g // 4, 0:piece, (g % 4) * width + lo:(g % 4) * width + lo + 256],
                              preferred_element_type=F32) for g in range(groups))
            x1 = (x_in[:, c * width + lo:c * width + lo + 256].astype(F32) + acc).astype(BF16)
            h_ref[c, :, lo:lo + 256] = x1
            x1 = x1.astype(F32)
            square += jnp.sum(x1 * x1, axis=-1, keepdims=True)
        if c + 2 < chunks:
            for g in range(groups):
                piece_copy(c + 2, g).start()
            if c == 1:
                weight(0).start()
        else:
            for i in (1, 2) if c % 2 == 0 else (3, 4):
                weight(i).start()
        push(2, c).start()
        push(4, c).start()
    inv = lax.rsqrt(square / d_model + NORM_EPS)
    meta_ref[2:3, :] = jnp.broadcast_to(inv, (tokens, tokens)).T[0:1]
    logits = jnp.zeros((tokens, n_experts), F32)
    for q in range(chunks):
        h2 = (h_ref[q].astype(F32) * inv * gain_ref[q * width:(q + 1) * width].astype(F32).reshape(1, -1)).astype(BF16)
        logits += lax.dot_general(h2, wr_ref[:, q * width:(q + 1) * width], (((1,), (1,)), ((), ())), preferred_element_type=F32)
    for r in (6, 2, 4, 7, 3, 5, 1):
        meta_copy(r).start()
    for q in range(chunks):
        push(1, q).start()
    lane = lax.broadcasted_iota(jnp.int32, logits.shape, 1).astype(F32) * cap
    own = [cols_ref[:, k:k + 1] for k in range(2)]
    p0, p1 = (jnp.sum(jnp.where((lane <= c) & (c < lane + cap), logits, 0.0), axis=-1, keepdims=True) for c in own)
    top = jnp.maximum(p0, p1)
    e0, e1 = jnp.exp(p0 - top), jnp.exp(p1 - top)
    gates_ref[:, 0:1] = e0 / (e0 + e1)
    gates_ref[:, 1:2] = e1 / (e0 + e1)

    slot_iota = lax.broadcasted_iota(jnp.int32, (local_experts * cap, tokens), 0)
    picks = {}

    def select(r, q):
        if r not in picks:
            if r:
                meta_copy(r).wait_recv()
            meta = meta_ref[...] if r == 0 else meta_in[r]
            want = (slot_iota + me * (local_experts * cap)).astype(F32)
            hit = (jnp.broadcast_to(meta[0:1], want.shape) == want) | (jnp.broadcast_to(meta[1:2], want.shape) == want)
            scale = jnp.sum(jnp.where(hit, jnp.broadcast_to(meta[2:3], want.shape), 0.0), axis=-1, keepdims=True)
            picks[r] = jnp.where(hit, 1.0, 0.0).astype(BF16), scale
        pick, scale = picks[r]
        got = jnp.dot(pick, block(r, q)[...], preferred_element_type=F32)
        got = (got * scale * gain_ref[q * width:(q + 1) * width].astype(F32).reshape(1, -1)).astype(BF16)
        for e in range(local_experts):
            x_ref[e, r * cap:(r + 1) * cap, q * width:(q + 1) * width] = got[e * cap:(e + 1) * cap]

    def y_copy(e, r):
        rows = pl.ds(r * cap, cap)
        return remote(x_ref.at[e, rows], y_in.at[e, rows], ysend.at[e, r], yrecv.at[e, r], r)

    def run_expert(e, lo_r, hi_r, slots, after_up=()):
        rows = slice(lo_r * cap, hi_r * cap)
        n_rows = (hi_r - lo_r) * cap
        for lo in range(0, d_ff, 256):
            hi = min(lo + 256, d_ff)
            gate, up = (lax.dot_general(x_ref[e, rows], wbuf[s, lo:hi], (((1,), (1,)), ((), ())), preferred_element_type=F32) for s in slots[:2])
            act_ref[0:n_rows, lo:hi] = (gate * jax.nn.sigmoid(gate) * up).astype(BF16)
        for i in after_up:
            weight(i).start()
        if e == 0 and lo_r == 0:
            weight(2).wait()
        if e == 1 and lo_r == 0:
            weight(5).wait()
        for lo in range(0, d_model, 512):
            x_ref[e, rows, lo:lo + 512] = jnp.dot(act_ref[0:n_rows], wbuf[slots[2], :, lo:lo + 512], preferred_element_type=F32).astype(BF16)

    for q in range(chunks):
        select(0, q)
    for q in range(chunks):
        for slot in (2, 4):
            push(slot, q).wait_recv()
            if (slot == 2) == (q < chunks // 2):
                push(6, q).start()
            push(slot + 1, q).start()
        for slot in (1, 2, 4):
            if slot == 1:
                push(slot, q).wait_recv()
            select(slot, q)
    for q in range(chunks):
        for slot in (3, 5):
            push(slot, q).wait_recv()
            select(slot, q)

    weight(0).wait()
    weight(1).wait()
    run_expert(0, 0, 6, (4, 0, 1), after_up=(5,))
    for r in (2, 4, 3, 5, 1):
        y_copy(0, r).start()
    y_in[0, 0:cap] = x_ref[0, 0:cap]
    weight(3).wait()
    weight(4).wait()
    run_expert(1, 0, 6, (2, 3, 4))
    for r in (2, 4, 3, 5, 1):
        y_copy(1, r).start()
    y_in[1, 0:cap] = x_ref[1, 0:cap]
    for q in (0, chunks // 2, 1, chunks // 2 + 1):
        push(6, q).wait_recv()
        push(7, q).start()
        select(6, q)
    for q in (0, chunks // 2, 1, chunks // 2 + 1):
        push(7, q).wait_recv()
        select(7, q)
    run_expert(1, 6, 8, (2, 3, 4), after_up=(6,))
    for r in (6, 7):
        y_copy(1, r).start()
    weight(6).wait()
    run_expert(0, 6, 8, (2, 0, 1))
    for r in (6, 7):
        y_copy(0, r).start()

    lane = lax.broadcasted_iota(jnp.int32, (tokens, rows_all), 1)
    rel, rank = lane // cap, lax.rem(lane, cap)
    owner = me + sum(lax.rem(rel // (1 << b), 2) * (1 << b) * (1 - 2 * bits[b]) for b in range(3))
    for e in (1, 0):
        for r in range(1, n_ep):
            y_copy(e, r).wait_recv()
        want = ((owner * local_experts + e) * cap + rank).astype(F32)
        sel = [jnp.where(cols_ref[:, k:k + 1] == want, 1.0, 0.0).astype(BF16) for k in range(2)]
        for lo in range(0, d_model, 512):
            y = y_in[e, :, lo:lo + 512]
            part = sum(gates_ref[:, k:k + 1] * jnp.dot(sel[k], y, preferred_element_type=F32) for k in range(2))
            if e:
                sum_ref[:, lo:lo + 512] = part
            else:
                x1 = h_ref[lo // width, :, lo % width:lo % width + 512].astype(F32)
                out_ref[:, lo:lo + 512] = (x1 + (sum_ref[:, lo:lo + 512] + part)).astype(BF16)

    for r in range(1, n_ep):
        meta_copy(r).wait_send()
        for q in range(chunks):
            push(r, q).wait_send()
        for e in range(local_experts):
            y_copy(e, r).wait_send()


def moe(hidden, mix, gain, w_router, expert_ids, w_out, w_gate, w_up, w_down, n_ep, cap):
    tokens, d_model = hidden.shape
    local_experts, d_ff, _ = w_down.shape
    vmem = pl.BlockSpec(memory_space=pltpu.VMEM)
    hbm = pl.BlockSpec(memory_space=pl.ANY)
    rows = n_ep * cap
    width = d_model // CHUNKS
    dma = pltpu.SemaphoreType.DMA
    return pl.pallas_call(
        functools.partial(moe_kernel, n_ep, n_ep * local_experts, cap),
        out_shape=jax.ShapeDtypeStruct((tokens, d_model), BF16),
        in_specs=[vmem] * 5 + [hbm] * 4,
        out_specs=vmem,
        scratch_shapes=[
            pltpu.VMEM((CHUNKS, tokens, width), BF16),
            pltpu.VMEM((n_ep - 1, CHUNKS, tokens, width), BF16),
            pltpu.VMEM((local_experts, rows, d_model), BF16),
            pltpu.VMEM((local_experts, rows, d_model), BF16),
            pltpu.VMEM((rows, d_ff), BF16),
            pltpu.VMEM((tokens, d_model), F32),
            pltpu.VMEM((tokens, 128), F32),
            pltpu.VMEM((tokens, 128), F32),
            pltpu.VMEM((8, tokens), F32),
            pltpu.VMEM((n_ep, 8, tokens), F32),
            pltpu.VMEM((5, d_ff, d_model), BF16),
            dma((16,)), dma((7,)), dma((n_ep,)), dma((n_ep,)), dma((n_ep, CHUNKS)), dma((n_ep, CHUNKS)),
            dma((local_experts, n_ep)), dma((local_experts, n_ep)),
        ],
        compiler_params=pltpu.CompilerParams(vmem_limit_bytes=67043328, collective_id=0, has_side_effects=True),
    )(hidden, mix, gain, w_router.T, expert_ids.T, w_out, jnp.swapaxes(w_gate, 1, 2), jnp.swapaxes(w_up, 1, 2), w_down)


def solution(mesh):
    n_ep = mesh.shape['ep']
    row_spec = P(('dp', 'ep'), None)
    cache_spec = P(('dp', 'ep'), None, None, None)
    expert_spec = P('ep', None, None)
    in_specs = (row_spec, cache_spec, cache_spec, P(('dp', 'ep')), row_spec, P(), P(), P(), P(), P(), P(), P(), expert_spec, expert_spec, expert_spec)
    out_specs = (row_spec, cache_spec, cache_spec)

    def device_step(hidden, k_cache, v_cache, seq_lens, expert_ids, attn_gain, w_query, w_key, w_value, w_out, ffn_gain, w_router, w_gate, w_up, w_down):
        tokens, d_model = hidden.shape
        local_experts = w_gate.shape[0]
        n_experts = local_experts * n_ep
        cap_slots = 4 * tokens // n_experts
        k_cache_new, v_cache_new, mix = attend(hidden, attn_gain, seq_lens, w_query, w_key, w_value, k_cache, v_cache)
        out = moe(hidden, mix, ffn_gain, w_router, expert_ids, w_out, w_gate, w_up, w_down, n_ep, cap_slots)
        return out, k_cache_new, v_cache_new

    return jax.shard_map(device_step, mesh=mesh, in_specs=in_specs, out_specs=out_specs, check_vma=False)
```

```python
import functools

import jax
import jax.numpy as jnp
from jax import lax
from jax.experimental import pallas as pl
from jax.experimental.pallas import tpu as pltpu
from jax.sharding import PartitionSpec as P

NORM_EPS = 1e-5
ROPE_THETA = 1000000.0
F32 = jnp.float32
BF16 = jnp.bfloat16
TILE = 256
RING = 12
CHUNKS = 4


def rms_rows(rows_f32, gain_row):
    inv_rms = lax.rsqrt(jnp.mean(rows_f32 * rows_f32, axis=-1, keepdims=True) + NORM_EPS)
    return (rows_f32 * inv_rms * gain_row).astype(BF16)


def attend_kernel(lens_ref, x_ref, gain_ref, freq_ref, wq, wk, wv, k_hbm, v_hbm, ko_hbm, vo_hbm, mix_ref,
                  h_ref, cos_ref, sin_ref, qkv_ref, o_ref, kc, vc, wbuf, wsems, in_sems, out_sems):
    tokens, seq_len, kv_heads, head_dim = kc.shape
    q_heads = wq.shape[1] // head_dim
    groups = q_heads // kv_heads
    spans = [w.shape[1] // TILE for w in (wq, wk, wv)]
    first = [0, spans[0], spans[0] + spans[1]]
    total = sum(spans)
    per_tile = TILE // head_dim
    n_parts = in_sems.shape[1]
    part = tokens // n_parts
    block = o_ref.shape[1]

    def cache_in(i, w):
        rows = pl.ds(i * part, part)
        return pltpu.make_async_copy((k_hbm, v_hbm)[w].at[rows], (kc, vc)[w].at[rows], in_sems.at[w, i])

    def cache_out(i, w):
        rows = pl.ds(i * part, part)
        return pltpu.make_async_copy((kc, vc)[w].at[rows], (ko_hbm, vo_hbm)[w].at[rows], out_sems.at[w, i])

    def start(t):
        slot = lax.rem(t, RING)
        for w, lo, n in zip((wq, wk, wv), first, spans):
            @pl.when((t >= lo) & (t < lo + n))
            def _():
                col = pl.multiple_of((t - lo) * TILE, TILE)
                pltpu.make_async_copy(w.at[:, pl.ds(col, TILE)], wbuf.at[slot], wsems.at[slot]).start()

        @pl.when((t >= total) & (t < total + n_parts))
        def _():
            for w in range(2):
                cache_in(t - total, w).start()

    for t in range(RING - 1):
        start(jnp.int32(t))
    h_ref[...] = rms_rows(x_ref[...].astype(F32), gain_ref[...].astype(F32).reshape(1, -1))

    def fill(t, carry):
        cos_ref[pl.ds(t, 1), :] = jnp.full((1, head_dim), lens_ref[t].astype(F32))
        return carry

    lax.fori_loop(0, tokens, fill, 0)
    angles = cos_ref[...] * freq_ref[...]
    lane = lax.broadcasted_iota(jnp.int32, angles.shape, 1)
    sines = jnp.sin(angles)
    cos_ref[...] = jnp.cos(angles)
    sin_ref[...] = jnp.where(lane < head_dim // 2, -sines, sines)

    def project(t, carry):
        slot = lax.rem(t, RING)
        start(t + RING - 1)
        pltpu.make_async_copy(wq.at[:, pl.ds(0, TILE)], wbuf.at[slot], wsems.at[slot]).wait()
        acc = jnp.dot(h_ref[...], wbuf[slot], preferred_element_type=F32)
        for i in range(per_tile):
            v = acc[:, i * head_dim:(i + 1) * head_dim].astype(BF16).astype(F32)
            rot = v * cos_ref[...] + pltpu.roll(v, head_dim // 2, 1) * sin_ref[...]
            qkv_ref[t * per_tile + i] = jnp.where(t < first[2], rot.astype(BF16).astype(F32), v)
        return carry

    lax.fori_loop(0, total, project, 0)

    cols = seq_len * kv_heads
    lane = lax.broadcasted_iota(jnp.int32, (q_heads, cols), 1)
    row = lax.broadcasted_iota(jnp.int32, (q_heads, cols), 0)
    pos = jnp.where(lax.rem(lane, kv_heads) == row // groups, lane // kv_heads, seq_len)
    flat = qkv_ref.reshape(qkv_ref.shape[0] * tokens, head_dim)
    o2 = o_ref.reshape(q_heads * block, head_dim)

    def heads_of(t, lo, n):
        return flat[pl.ds(lo * tokens + t, n, stride=tokens), :].astype(BF16)

    def attend_part(i, carry):
        for w in range(2):
            cache_in(i, w).wait()
        for b in range(part // block):
            base = i * part + b * block
            lens = [lens_ref[base + t] for t in range(block)]
            for t in range(block):
                kc[base + t, lens[t]] = heads_of(base + t, q_heads, kv_heads)
                vc[base + t, lens[t]] = heads_of(base + t, q_heads + kv_heads, kv_heads)
            scores = [lax.dot_general(heads_of(base + t, 0, q_heads), kc[base + t].reshape(cols, head_dim),
                                      (((1,), (1,)), ((), ())), preferred_element_type=F32) for t in range(block)]
            probs = []
            for t in range(block):
                s = jnp.where(pos <= lens[t], scores[t] * head_dim ** -0.5, -jnp.inf)
                e = jnp.exp(s - jnp.max(s, axis=-1, keepdims=True))
                probs.append((e / jnp.sum(e, axis=-1, keepdims=True)).astype(BF16))
            for t in range(block):
                o2[pl.ds(t, q_heads, stride=block), :] = jnp.dot(probs[t], vc[base + t].reshape(cols, head_dim), preferred_element_type=F32)
            rows = pl.ds(pl.multiple_of(base, block), block)
            for j in range(q_heads):
                mix_ref[rows, j * head_dim:(j + 1) * head_dim] = o_ref[j].astype(BF16)
        for w in range(2):
            cache_out(i, w).start()
        return carry

    for t in range(total + RING - 1, total + n_parts):
        start(jnp.int32(t))
    lax.fori_loop(0, n_parts, attend_part, 0)
    for i in range(n_parts):
        for w in range(2):
            cache_out(i, w).wait()


def attend(hidden, gain, positions, wq, wk, wv, k_cache, v_cache):
    tokens, d_model = hidden.shape
    seq_len, kv_heads, head_dim = k_cache.shape[1:]
    q_dim = wq.shape[1]
    q_heads = q_dim // head_dim
    half_dim = head_dim // 2
    inv_freq = ROPE_THETA ** (-2.0 * jnp.arange(half_dim, dtype=F32) / head_dim)
    freq = jnp.concatenate([inv_freq, inv_freq]).reshape(1, head_dim)
    parts, block = 8, 8
    vmem = pl.BlockSpec(memory_space=pltpu.VMEM)
    hbm = pl.BlockSpec(memory_space=pl.ANY)
    dma = pltpu.SemaphoreType.DMA
    return pl.pallas_call(
        attend_kernel,
        out_shape=[jax.ShapeDtypeStruct(k_cache.shape, BF16), jax.ShapeDtypeStruct(v_cache.shape, BF16),
                   jax.ShapeDtypeStruct((tokens, q_dim), BF16)],
        in_specs=[pl.BlockSpec(memory_space=pltpu.SMEM), vmem, vmem, vmem] + [hbm] * 5,
        out_specs=[hbm, hbm, vmem],
        scratch_shapes=[
            pltpu.VMEM((tokens, d_model), BF16), pltpu.VMEM((tokens, head_dim), F32), pltpu.VMEM((tokens, head_dim), F32),
            pltpu.VMEM((q_heads + 2 * kv_heads, tokens, head_dim), F32), pltpu.VMEM((q_heads, block, head_dim), F32),
            pltpu.VMEM(k_cache.shape, BF16), pltpu.VMEM(v_cache.shape, BF16),
            pltpu.VMEM((RING, d_model, TILE), BF16),
            dma((RING,)), dma((2, parts)), dma((2, parts)),
        ],
        compiler_params=pltpu.CompilerParams(vmem_limit_bytes=67043328),
    )(positions, hidden, gain, freq, wq, wk, wv, k_cache, v_cache)


def moe_kernel(n_ep, n_dp, n_experts, cap, x_in, mix_ref, gain_ref, wr_ref, ids_ref, wo, wg, wu, wd, out_ref, gates_ref, cols_ref, flag_out, spill,
               h_ref, buf, x_ref, y_first, y_rest, act_ref, meta_ref, meta_in, flag_ref, flag_in, wbuf,
               osem, wsem, csend, crecv, gsend, grecv, ysend, yrecv, fsend, frecv, ssem):
    me = lax.axis_index('ep')
    group = lax.axis_index('dp')
    half = cap // 2
    bits = [lax.rem(me, 2), lax.rem(me // 2, 2), me // 4]
    chunks, tokens, width = h_ref.shape
    d_model = chunks * width
    local_experts, rows_all, _ = x_ref.shape
    d_ff = wd.shape[1]
    q_dim = wo.shape[0]

    def peer(r):
        return me + sum(((r >> b) & 1) * (1 << b) * (1 - 2 * bits[b]) for b in range(3))

    def remote(src, dst, send, recv, r):
        return pltpu.make_async_remote_copy(src_ref=src, dst_ref=dst, send_sem=send, recv_sem=recv, device_id={'ep': peer(r)},
                                            device_id_type=pl.DeviceIdType.MESH)

    def block(r, q):
        return h_ref.at[q] if r == 0 else buf.at[r - 1, q]

    def push(slot, q):
        if slot in (2, 4):
            src, to = 0, slot
        elif slot == 6:
            src, to = (2, 4) if q < chunks // 2 else (4, 2)
        else:
            src, to = slot - 1, 1
        return remote(block(src, q), buf.at[slot - 1, q], gsend.at[slot, q], grecv.at[slot, q], to)

    groups = 8
    piece = q_dim // groups

    def piece_at(c, g):
        return wbuf.at[2 * (c % 2) + g // 4, 0:piece, (g % 4) * width:(g % 4 + 1) * width]

    def piece_copy(c, g):
        return pltpu.make_async_copy(wo.at[g * piece:(g + 1) * piece, c * width:(c + 1) * width], piece_at(c, g), osem.at[(c % 2) * groups + g])

    loads = ((0, 0, 4), (1, 0, 0), (2, 0, 1), (0, 1, 2), (1, 1, 3), (2, 1, 4), (0, 0, 2))

    def weight(i):
        m, e, slot = loads[i]
        return pltpu.make_async_copy((wg, wu, wd)[m].at[e], wbuf.at[slot], wsem.at[i])

    def flag_copy(d):
        return pltpu.make_async_remote_copy(src_ref=flag_ref, dst_ref=flag_in.at[d], send_sem=fsend.at[d], recv_sem=frecv.at[d],
                                            device_id={'dp': lax.rem(group + d, n_dp)}, device_id_type=pl.DeviceIdType.MESH)

    def meta_copy(r):
        return remote(meta_ref, meta_in.at[r], csend.at[r], crecv.at[r], r)

    for c in range(2):
        for g in range(groups):
            piece_copy(c, g).start()
    barrier = pltpu.get_barrier_semaphore()
    for r in range(1, n_ep):
        pl.semaphore_signal(barrier, inc=1, device_id={'ep': peer(r)}, device_id_type=pl.DeviceIdType.MESH)
    for d in range(1, n_dp):
        pl.semaphore_signal(barrier, inc=1, device_id={'dp': lax.rem(group + d, n_dp)}, device_id_type=pl.DeviceIdType.MESH)

    expert = lax.broadcasted_iota(jnp.int32, (n_experts, tokens), 0)
    hits = [jnp.where(jnp.broadcast_to(ids_ref[k:k + 1, :], expert.shape) == expert, 1.0, 0.0) for k in range(2)]
    earlier = lax.broadcasted_iota(jnp.int32, (tokens, tokens), 0) < lax.broadcasted_iota(jnp.int32, (tokens, tokens), 1)
    before = jnp.dot((hits[0] + hits[1]).astype(BF16), jnp.where(earlier, 1.0, 0.0).astype(BF16), preferred_element_type=F32)
    code = [ids_ref[k:k + 1, :].astype(F32) * cap + jnp.sum(hits[k] * before, axis=0, keepdims=True) for k in range(2)]
    counts = jnp.broadcast_to(jnp.sum(hits[0] + hits[1], axis=1, keepdims=True), before.shape)
    odd = lax.rem(expert, 2)
    off_x, off_y = lax.rem(expert // 4, 2), expert // 8
    off_x = off_x + bits[1] - 2 * off_x * bits[1]
    off_y = off_y + bits[2] - 2 * off_y * bits[2]
    first = lax.rem(odd + off_x * off_y, 2) == 0
    other = jnp.where(odd == 0, pltpu.roll(counts, n_experts - 1, 0), pltpu.roll(counts, 1, 0))
    device = (expert // 2).astype(F32)
    later = jnp.where(first, before - half + other, before)
    place = jnp.where(first & (before < half), device * half + before, n_ep * cap + device * (2 * cap) + later)
    over = jnp.where(first & (before < half), 0.0, jnp.where(later >= cap, 1.0, 0.0))
    places = [jnp.sum(hits[k] * place, axis=0, keepdims=True) for k in range(2)]
    spilled = jnp.max(jnp.max((hits[0] + hits[1]) * over, axis=0, keepdims=True), axis=1, keepdims=True)
    zero = jnp.zeros((1, tokens), F32)
    meta_ref[...] = jnp.concatenate(code + [zero] + places + [zero + spilled, zero, zero], axis=0)
    cols_ref[...] = jnp.concatenate([meta_ref[...]] * (tokens // 8), axis=0).T

    pl.semaphore_wait(barrier, n_ep + n_dp - 2)

    square = jnp.zeros((tokens, 1), F32)
    for c in range(chunks):
        for g in range(groups):
            piece_copy(c, g).wait()
        for lo in range(0, width, 256):
            acc = sum(jnp.dot(mix_ref[:, g * piece:(g + 1) * piece],
                              wbuf[2 * (c % 2) + g // 4, 0:piece, (g % 4) * width + lo:(g % 4) * width + lo + 256],
                              preferred_element_type=F32) for g in range(groups))
            x1 = (x_in[:, c * width + lo:c * width + lo + 256].astype(F32) + acc).astype(BF16)
            h_ref[c, :, lo:lo + 256] = x1
            x1 = x1.astype(F32)
            square += jnp.sum(x1 * x1, axis=-1, keepdims=True)
        if c + 2 < chunks:
            for g in range(groups):
                piece_copy(c + 2, g).start()
            if c == 1:
                weight(0).start()
        else:
            for i in (1, 2) if c % 2 == 0 else (3, 4):
                weight(i).start()
        push(2, c).start()
        push(4, c).start()
    inv = lax.rsqrt(square / d_model + NORM_EPS)
    meta_ref[2:3, :] = jnp.broadcast_to(inv, (tokens, tokens)).T[0:1]
    logits = jnp.zeros((tokens, n_experts), F32)
    for q in range(chunks):
        h2 = (h_ref[q].astype(F32) * inv * gain_ref[q * width:(q + 1) * width].astype(F32).reshape(1, -1)).astype(BF16)
        logits += lax.dot_general(h2, wr_ref[:, q * width:(q + 1) * width], (((1,), (1,)), ((), ())), preferred_element_type=F32)
    for r in (6, 2, 4, 7, 3, 5, 1):
        meta_copy(r).start()
    for q in range(chunks):
        push(1, q).start()
    lane = lax.broadcasted_iota(jnp.int32, logits.shape, 1).astype(F32) * cap
    own = [cols_ref[:, k:k + 1] for k in range(2)]
    p0, p1 = (jnp.sum(jnp.where((lane <= c) & (c < lane + cap), logits, 0.0), axis=-1, keepdims=True) for c in own)
    top = jnp.maximum(p0, p1)
    e0, e1 = jnp.exp(p0 - top), jnp.exp(p1 - top)
    gates_ref[:, 0:1] = e0 / (e0 + e1)
    gates_ref[:, 1:2] = e1 / (e0 + e1)

    slot_iota = lax.broadcasted_iota(jnp.int32, (local_experts * cap, tokens), 0)
    picks = {}

    def select(r, q):
        if r not in picks:
            if r:
                meta_copy(r).wait_recv()
            meta = meta_ref[...] if r == 0 else meta_in[r]
            want = (slot_iota + me * (local_experts * cap)).astype(F32)
            hit = (jnp.broadcast_to(meta[0:1], want.shape) == want) | (jnp.broadcast_to(meta[1:2], want.shape) == want)
            scale = jnp.sum(jnp.where(hit, jnp.broadcast_to(meta[2:3], want.shape), 0.0), axis=-1, keepdims=True)
            picks[r] = jnp.where(hit, 1.0, 0.0).astype(BF16), scale
        pick, scale = picks[r]
        got = jnp.dot(pick, block(r, q)[...], preferred_element_type=F32)
        got = (got * scale * gain_ref[q * width:(q + 1) * width].astype(F32).reshape(1, -1)).astype(BF16)
        for e in range(local_experts):
            x_ref[e, r * cap:(r + 1) * cap, q * width:(q + 1) * width] = got[e * cap:(e + 1) * cap]

    def y_copy(p, r):
        rows = pl.ds(r * cap, half if p == 0 else cap)
        dst = y_first.at[pl.ds(r * half, half)] if p == 0 else y_rest.at[pl.ds(r * cap, cap)]
        return remote(x_ref.at[p if r < 6 else 1 - p, rows], dst, ysend.at[p, r], yrecv.at[p, r], r)

    def compact(r):
        f = int(r >= 6)
        meta = meta_ref[...] if r == 0 else meta_in[r]
        lo = ((me * 2 + 1 - f) * cap).astype(F32)
        mine = jnp.where((meta[0:2] >= lo) & (meta[0:2] < lo + cap), 1.0, 0.0)
        n_odd = jnp.sum(jnp.sum(mine, axis=0, keepdims=True), axis=1, keepdims=True)
        shape = (cap + half, 2 * cap)
        to = lax.broadcasted_iota(jnp.int32, shape, 0).astype(F32)
        frm = lax.broadcasted_iota(jnp.int32, shape, 1).astype(F32)
        count = jnp.broadcast_to(n_odd, shape)
        odd = (frm >= cap) & (frm - cap < count) & (to == frm - cap)
        rest = (frm >= half) & (frm < cap) & (to == frm - half + count)
        move = jnp.where(odd | rest, 1.0, 0.0).astype(BF16)
        rows = slice(r * cap, (r + 1) * cap)
        for lo in range(0, d_model, 512):
            y = jnp.concatenate([x_ref[f, rows, lo:lo + 512], x_ref[1 - f, rows, lo:lo + 512]], axis=0)
            z = jnp.dot(move, y, preferred_element_type=F32).astype(BF16)
            x_ref[1 - f, rows, lo:lo + 512] = z[:cap]
            x_ref[f, r * cap + half:(r + 1) * cap, lo:lo + 512] = z[cap:]

    def spill_copy(r):
        return pltpu.make_async_copy(x_ref.at[int(r >= 6), pl.ds(r * cap + half, half)], spill.at[peer(r)], ssem.at[r])

    def run_expert(e, lo_r, hi_r, slots, after_up=()):
        rows = slice(lo_r * cap, hi_r * cap)
        n_rows = (hi_r - lo_r) * cap
        for lo in range(0, d_ff, 256):
            hi = min(lo + 256, d_ff)
            gate, up = (lax.dot_general(x_ref[e, rows], wbuf[s, lo:hi], (((1,), (1,)), ((), ())), preferred_element_type=F32) for s in slots[:2])
            act_ref[0:n_rows, lo:hi] = (gate * jax.nn.sigmoid(gate) * up).astype(BF16)
        for i in after_up:
            weight(i).start()
        if e == 0 and lo_r == 0:
            weight(2).wait()
        if e == 1 and lo_r == 0:
            weight(5).wait()
        for lo in range(0, d_model, 512):
            x_ref[e, rows, lo:lo + 512] = jnp.dot(act_ref[0:n_rows], wbuf[slots[2], :, lo:lo + 512], preferred_element_type=F32).astype(BF16)

    for q in range(chunks):
        select(0, q)
    for q in range(chunks):
        for slot in (2, 4):
            push(slot, q).wait_recv()
            if (slot == 2) == (q < chunks // 2):
                push(6, q).start()
            push(slot + 1, q).start()
        for slot in (1, 2, 4):
            if slot == 1:
                push(slot, q).wait_recv()
            select(slot, q)
    for q in range(chunks):
        for slot in (3, 5):
            push(slot, q).wait_recv()
            select(slot, q)

    weight(0).wait()
    weight(1).wait()
    run_expert(0, 0, 6, (4, 0, 1), after_up=(5,))
    for r in (2, 4, 3, 5, 1):
        y_copy(0, r).start()
    y_first[0:half] = x_ref[0, 0:half]
    weight(3).wait()
    weight(4).wait()
    run_expert(1, 0, 6, (2, 3, 4))
    for r in (2, 4, 3, 5, 1):
        compact(r)
        y_copy(1, r).start()
    compact(0)
    y_rest[0:cap] = x_ref[1, 0:cap]
    for q in (0, chunks // 2, 1, chunks // 2 + 1):
        push(6, q).wait_recv()
        push(7, q).start()
        select(6, q)
    for q in (0, chunks // 2, 1, chunks // 2 + 1):
        push(7, q).wait_recv()
        select(7, q)
    run_expert(1, 6, 8, (2, 3, 4), after_up=(6,))
    for r in (6, 7):
        y_copy(0, r).start()
    weight(6).wait()
    run_expert(0, 6, 8, (2, 0, 1))
    for r in (6, 7):
        compact(r)
        y_copy(1, r).start()
    flag = meta_ref[5:6]
    for r in range(1, n_ep):
        flag = jnp.maximum(flag, meta_in[r, 5:6])
    flag_ref[...] = jnp.broadcast_to(flag, flag_ref.shape)
    for d in range(1, n_dp):
        flag_copy(d).start()
    for r in range(n_ep):
        spill_copy(r).start()

    for p, per, y_ref in ((0, half, y_first), (1, cap, y_rest)):
        lane = lax.broadcasted_iota(jnp.int32, (tokens, n_ep * per), 1)
        rel, rank = lane // per, lax.rem(lane, per)
        owner = me + sum(lax.rem(rel // (1 << b), 2) * (1 << b) * (1 - 2 * bits[b]) for b in range(3))
        want = (owner * half + rank if p == 0 else n_ep * cap + owner * (2 * cap) + rank).astype(F32)
        sel = [jnp.where(cols_ref[:, 3 + k:4 + k] == want, 1.0, 0.0).astype(BF16) for k in range(2)]
        for r in range(1, n_ep):
            y_copy(p, r).wait_recv()
        for lo in range(0, d_model, 512):
            y = y_ref[:, lo:lo + 512]
            part = sum(gates_ref[:, k:k + 1] * jnp.dot(sel[k], y, preferred_element_type=F32) for k in range(2))
            if p == 0:
                out_ref[:, lo:lo + 512] = part
            else:
                x1 = h_ref[lo // width, :, lo % width:lo % width + 512].astype(F32)
                out_ref[:, lo:lo + 512] = x1 + (out_ref[:, lo:lo + 512] + part)

    flag = flag_ref[...]
    for d in range(1, n_dp):
        flag_copy(d).wait_recv()
        flag = jnp.maximum(flag, flag_in[d])
    flag_out[...] = flag
    for d in range(1, n_dp):
        flag_copy(d).wait_send()
    for r in range(n_ep):
        spill_copy(r).wait()
    for r in range(1, n_ep):
        meta_copy(r).wait_send()
        for q in range(chunks):
            push(r, q).wait_send()
        for e in range(local_experts):
            y_copy(e, r).wait_send()


def moe(hidden, mix, gain, w_router, expert_ids, w_out, w_gate, w_up, w_down, n_ep, n_dp, cap):
    tokens, d_model = hidden.shape
    local_experts, d_ff, _ = w_down.shape
    half = cap // 2
    vmem = pl.BlockSpec(memory_space=pltpu.VMEM)
    hbm = pl.BlockSpec(memory_space=pl.ANY)
    rows = n_ep * cap
    width = d_model // CHUNKS
    dma = pltpu.SemaphoreType.DMA
    total, gates, cols, flag, spill = pl.pallas_call(
        functools.partial(moe_kernel, n_ep, n_dp, n_ep * local_experts, cap),
        out_shape=[jax.ShapeDtypeStruct((tokens, d_model), F32), jax.ShapeDtypeStruct((tokens, 128), F32), jax.ShapeDtypeStruct((tokens, 128), F32),
                   jax.ShapeDtypeStruct((8, tokens), F32), jax.ShapeDtypeStruct((n_ep, half, d_model), BF16)],
        in_specs=[vmem] * 5 + [hbm] * 4,
        out_specs=[vmem] * 4 + [hbm],
        scratch_shapes=[
            pltpu.VMEM((CHUNKS, tokens, width), BF16),
            pltpu.VMEM((n_ep - 1, CHUNKS, tokens, width), BF16),
            pltpu.VMEM((local_experts, rows, d_model), BF16),
            pltpu.VMEM((n_ep * half, d_model), BF16),
            pltpu.VMEM((n_ep * cap, d_model), BF16),
            pltpu.VMEM((rows, d_ff), BF16),
            pltpu.VMEM((8, tokens), F32),
            pltpu.VMEM((n_ep, 8, tokens), F32),
            pltpu.VMEM((8, tokens), F32),
            pltpu.VMEM((n_dp, 8, tokens), F32),
            pltpu.VMEM((5, d_ff, d_model), BF16),
            dma((16,)), dma((7,)), dma((n_ep,)), dma((n_ep,)), dma((n_ep, CHUNKS)), dma((n_ep, CHUNKS)),
            dma((2, n_ep)), dma((2, n_ep)), dma((n_dp,)), dma((n_dp,)), dma((n_ep,)),
        ],
        compiler_params=pltpu.CompilerParams(vmem_limit_bytes=67043328, collective_id=0, has_side_effects=True),
    )(hidden, mix, gain, w_router.T, expert_ids.T, w_out, jnp.swapaxes(w_gate, 1, 2), jnp.swapaxes(w_up, 1, 2), w_down)

    def with_spill(total, gates, cols, spill):
        rows_in = lax.all_to_all(spill, 'ep', 0, 0, tiled=True).reshape(n_ep * half, d_model)
        at = jnp.arange(n_ep * half)
        want = (n_ep * cap + at // half * (2 * cap) + cap + at % half).astype(F32)
        for k in range(2):
            sel = (cols[:, 3 + k:4 + k] == want).astype(BF16)
            total = total + gates[:, k:k + 1] * jnp.dot(sel, rows_in, preferred_element_type=F32)
        return total.astype(BF16)

    return lax.cond(flag[0, 0] > 0, with_spill, lambda total, gates, cols, spill: total.astype(BF16), total, gates, cols, spill)


def solution(mesh):
    n_ep = mesh.shape['ep']
    row_spec = P(('dp', 'ep'), None)
    cache_spec = P(('dp', 'ep'), None, None, None)
    expert_spec = P('ep', None, None)
    in_specs = (row_spec, cache_spec, cache_spec, P(('dp', 'ep')), row_spec, P(), P(), P(), P(), P(), P(), P(), expert_spec, expert_spec, expert_spec)
    out_specs = (row_spec, cache_spec, cache_spec)

    def device_step(hidden, k_cache, v_cache, seq_lens, expert_ids, attn_gain, w_query, w_key, w_value, w_out, ffn_gain, w_router, w_gate, w_up, w_down):
        tokens, d_model = hidden.shape
        local_experts = w_gate.shape[0]
        n_experts = local_experts * n_ep
        cap_slots = 4 * tokens // n_experts
        k_cache_new, v_cache_new, mix = attend(hidden, attn_gain, seq_lens, w_query, w_key, w_value, k_cache, v_cache)
        out = moe(hidden, mix, ffn_gain, w_router, expert_ids, w_out, w_gate, w_up, w_down, n_ep, mesh.shape['dp'], cap_slots)
        return out, k_cache_new, v_cache_new

    return jax.shard_map(device_step, mesh=mesh, in_specs=in_specs, out_specs=out_specs, check_vma=False)
```
